32 devices in a mesh: gx: 2 (over x), gy: 4 (over y, core), gz: 4 (over z).
Axes of the slice: x: 2, y: 2, z: 4, core: 2. Of those that a mesh axis runs over, the one named last changes fastest.
Arguments:
- ref_pos: float32 [2, 4, 4, 3, 20480], P('gx', 'gy', 'gz'), may hold values from -6 to 6
- step: float32 [2, 4, 4, 3, 20480], P('gx', 'gy', 'gz'), may hold values from -6 to 6
- inv_mass: float32 [2, 4, 4, 20480], P('gx', 'gy', 'gz'), may hold values from 0.08 to 1
- boundary: int32 [2, 4, 4, 1], P('gx', 'gy', 'gz'), may hold values from 0 to 18432, as said below
- bonds: int32 [2, 4, 4, 2, 24416], P('gx', 'gy', 'gz'), may hold values from 0 to 75775, as said below
Outputs:
- positions: float32 [2, 4, 4, 3, 20480], P('gx', 'gy', 'gz')
- max_deviation: float32 [3], replicated
The draws below stay inside these ranges and needn't reach their ends.
Inputs may be any that keep to these rules, and one draw needn't show every extreme that they name: Each domain's boundary atoms are the 2048 consecutive atoms from boundary on; boundary is a multiple of 2048. In each domain bond c * 127 + m, for the first 20320 bonds, joins atom 128 * c + m to atom 128 * c + m + 1 (chains of 128 consecutive atoms). Cross bond k (bond 20320 + k) joins the domain's boundary atom boundary + (k mod 2048) (first row) to entry k mod 2048 of one of the 26 neighbour blocks of the extended list (second row), never the centre block; which blocks are reached, and how many bonds each one receives, varies from domain to domain. Every such bond is also listed by that neighbour domain with its two ends swapped, the domain's atom then standing in the neighbour's opposite block.
All inputs are finite; a program needn't handle non-finite values.
Results may differ from the reference program's by a relative error of at most 0.00018.
Values sent between devices are 32-bit elements; how exact they have to be, the bound alone decides.
A program may use at most 64 MiB of HBM per device.

```python
import math
import jax
import jax.numpy as jnp

ATOMS_DEV = 20480
BOUND = 2048
CROSS_BONDS = 4096
ITERS = 3
LOCAL_BONDS = 20320
N_GX = 2
N_GY = 4
N_GZ = 4


def draw_step(key, part):
    domains = N_GX * N_GY * N_GZ
    first_key, second_key = jax.random.split(key, 2)
    flat = jnp.arange(domains, dtype=jnp.float32).reshape(N_GX, N_GY, N_GZ, 1, 1) / max(domains - 1, 1)
    level = 0.1 * (1.0 + 2.0 * flat)
    factor = jnp.exp(jax.random.uniform(second_key, (N_GX, N_GY, N_GZ, 1, ATOMS_DEV), jnp.float32, jnp.log(0.5), jnp.log(2.0)))
    noise = jax.random.normal(first_key, (N_GX, N_GY, N_GZ, 3, ATOMS_DEV), jnp.float32)
    values = noise * level * factor
    return jnp.clip(values, -6.0, 6.0).astype(jnp.float32)


def boundary_start(key):
    runs = ATOMS_DEV // BOUND
    start = jax.random.randint(jax.random.fold_in(key, 11), (N_GX, N_GY, N_GZ, 1), 0, runs)
    return (start * BOUND).astype(jnp.int32)


def draw_boundary(key, part):
    return boundary_start(key)


def forced_phase(phase_now, coord, leaning):
    return jnp.where(leaning != 0, (coord + (leaning < 0).astype(jnp.int32)) % 2, phase_now).astype(jnp.int32)


def pair_number(coord, phase, extent):
    return ((coord - phase) % extent // 2).astype(jnp.int32)


def axis_moves(placed, switches, axis):
    swapped = jnp.take_along_axis(switches, (placed // 2).astype(jnp.int32), axis=axis)
    return (swapped * (1 - 2 * (placed % 2))).astype(jnp.int32)


def draw_bonds(key, part):
    grid = (N_GX, N_GY, N_GZ)
    domains = N_GX * N_GY * N_GZ
    start = boundary_start(key)
    chains = jnp.arange(ATOMS_DEV, dtype=jnp.int32).reshape(ATOMS_DEV // 128, 128)
    local_left = jnp.broadcast_to(chains[:, :-1].reshape(LOCAL_BONDS), grid + (LOCAL_BONDS,))
    local_right = jnp.broadcast_to(chains[:, 1:].reshape(LOCAL_BONDS), grid + (LOCAL_BONDS,))
    half = CROSS_BONDS // 2
    bond_rows = jnp.arange(half, dtype=jnp.int32)
    focus = jax.random.randint(jax.random.fold_in(key, 41), (), 0, domains).astype(jnp.int32)
    focus_x = focus // (N_GY * N_GZ)
    focus_y = focus // N_GZ % N_GY
    focus_z = focus % N_GZ
    chosen = jax.random.randint(jax.random.fold_in(key, 43), (), 0, 26).astype(jnp.int32)
    chosen = chosen + (chosen >= 13).astype(jnp.int32)
    lean_x = chosen // 9 - 1
    lean_y = chosen // 3 % 3 - 1
    lean_z = chosen % 3 - 1
    coord_z = jnp.arange(N_GZ, dtype=jnp.int32)
    phase_z = jax.random.randint(jax.random.fold_in(key, 47), (half,), 0, 2).astype(jnp.int32)
    phase_z = forced_phase(phase_z, focus_z, lean_z)
    switch_z = jax.random.randint(jax.random.fold_in(key, 53), (half, N_GZ // 2), 0, 2).astype(jnp.int32)
    switch_z = switch_z.at[bond_rows, pair_number(focus_z, phase_z, N_GZ)].set((lean_z != 0).astype(jnp.int32))
    placed_z = (coord_z[None, :] - phase_z[:, None]) % N_GZ
    offset_z = axis_moves(placed_z, switch_z, 1)
    coord_y = jnp.arange(N_GY, dtype=jnp.int32)
    phase_y = jax.random.randint(jax.random.fold_in(key, 59), (half, N_GZ), 0, 2).astype(jnp.int32)
    phase_y = phase_y.at[:, focus_z].set(forced_phase(phase_y[:, focus_z], focus_y, lean_y))
    switch_y = jax.random.randint(jax.random.fold_in(key, 61), (half, N_GZ, N_GY // 2), 0, 2).astype(jnp.int32)
    switch_y = switch_y.at[bond_rows, focus_z, pair_number(focus_y, phase_y[:, focus_z], N_GY)].set((lean_y != 0).astype(jnp.int32))
    placed_y = (coord_y[None, None, :] - phase_y[:, :, None]) % N_GY
    offset_y = axis_moves(placed_y, switch_y, 2)
    coord_x = jnp.arange(N_GX, dtype=jnp.int32)
    phase_x = jax.random.randint(jax.random.fold_in(key, 67), (half, N_GZ, N_GY), 0, 2).astype(jnp.int32)
    phase_x = phase_x.at[:, focus_z, focus_y].set(forced_phase(phase_x[:, focus_z, focus_y], focus_x, lean_x))
    switch_x = jax.random.randint(jax.random.fold_in(key, 71), (half, N_GZ, N_GY, N_GX // 2), 0, 2).astype(jnp.int32)
    standing = (offset_z[:, :, None] == 0) & (offset_y == 0)
    switch_x = jnp.where(standing[..., None], 1, switch_x).astype(jnp.int32)
    switch_x = switch_x.at[bond_rows, focus_z, focus_y, pair_number(focus_x, phase_x[:, focus_z, focus_y], N_GX)].set((lean_x != 0).astype(jnp.int32))
    placed_x = (coord_x[None, None, None, :] - phase_x[..., None]) % N_GX
    offset_x = axis_moves(placed_x, switch_x, 3)
    move_x = jnp.transpose(offset_x, (0, 3, 2, 1))
    move_y = jnp.transpose(offset_y, (0, 2, 1))[:, None, :, :]
    move_z = offset_z[:, None, None, :]
    first_block = (move_x + 1) * 9 + (move_y + 1) * 3 + (move_z + 1)
    first_block = jnp.broadcast_to(first_block, (half,) + grid).astype(jnp.int32)
    grid_x = coord_x[None, :, None, None]
    grid_y = coord_y[None, None, :, None]
    grid_z = coord_z[None, None, None, :]
    target = ((grid_x + move_x) % N_GX * N_GY + (grid_y + move_y) % N_GY) * N_GZ + (grid_z + move_z) % N_GZ
    target_flat = jnp.broadcast_to(target, (half,) + grid).reshape(half, domains).astype(jnp.int32)
    first_flat = first_block.reshape(half, domains)
    mirror_flat = jnp.zeros((half, domains), jnp.int32).at[bond_rows[:, None], target_flat].set(26 - first_flat)
    first_dom = jnp.transpose(first_flat.reshape((half,) + grid), (1, 2, 3, 0))
    mirror_dom = jnp.transpose(mirror_flat.reshape((half,) + grid), (1, 2, 3, 0))
    slot = bond_rows % BOUND
    own_left = jnp.broadcast_to(start + slot[None, None, None, :], grid + (half,))
    root_right = ATOMS_DEV + first_dom * BOUND + slot[None, None, None, :]
    mirror_right = ATOMS_DEV + mirror_dom * BOUND + slot[None, None, None, :]
    left_atom = jnp.concatenate([local_left, own_left, own_left], axis=3)
    right_atom = jnp.concatenate([local_right, root_right, mirror_right], axis=3)
    return jnp.stack([left_atom, right_atom], axis=3).astype(jnp.int32)


def levels(key, shape, cuts, low, high):
    factor_of, own = 1.0, jax.random.fold_in(key, 6)
    for position, shards_of in cuts:
        heights = jnp.exp(jax.random.uniform(jax.random.fold_in(own, position), (shards_of,), jnp.float32, low / len(cuts), high / len(cuts)))
        factor_of = factor_of * jnp.repeat(heights, shape[position] // shards_of).reshape([-1 if axis == position else 1 for axis in range(len(shape))])
    return factor_of


def centred(rng, dims, scale, most, pieces=(), kind=jnp.bfloat16):
    array = scale * jax.random.normal(rng, dims, jnp.float32)
    if pieces:
        array = array * levels(rng, dims, pieces, -0.22, 0.18)
    return jnp.clip(array, -most, most).astype(kind)


def setup_inputs(seed: int = 0) -> dict:
    key_list = jax.random.split(jax.random.key(seed), 6)
    ref_pos = centred(key_list[0], (N_GX, N_GY, N_GZ, 3, ATOMS_DEV), 1.0, 6.0, ((0, 2), (1, 4), (2, 4)), jnp.float32)
    step = draw_step(jax.random.fold_in(key_list[5], 71), 0)
    inv_mass = jnp.clip(jnp.exp(math.log(1.0) - 2.5257287 * jax.random.uniform(key_list[2], (N_GX, N_GY, N_GZ, ATOMS_DEV), jnp.float32) ** levels(key_list[2], (N_GX, N_GY, N_GZ, ATOMS_DEV), ((0, 2), (1, 4), (2, 4)), -0.2, 0.2)), 0.08, 1.0)
    boundary = draw_boundary(jax.random.fold_in(key_list[5], 71), 0)
    bonds = draw_bonds(jax.random.fold_in(key_list[5], 71), 0)
    return dict(ref_pos=ref_pos, step=step, inv_mass=inv_mass, boundary=boundary, bonds=bonds)


relax_factor = 0.7


def bond_terms(anchor_left, anchor_right, moved_left, moved_right, inverse_left, inverse_right):
    bond_rest = anchor_left - anchor_right
    bond_now = moved_left - moved_right
    rest_sq = jnp.sum(bond_rest * bond_rest, axis=0)
    now_sq = jnp.sum(bond_now * bond_now, axis=0)
    inner = jnp.sum(bond_rest * bond_now, axis=0)
    excess = now_sq - rest_sq
    deviation = jnp.max(jnp.abs(excess) / (2.0 * jnp.maximum(rest_sq, 1.0)))
    factor = relax_factor * excess / (2.0 * (inverse_left + inverse_right) * jnp.maximum(inner, 1.0))
    return factor * bond_rest, deviation


def apply_terms(current, shift_term, left_atom, right_atom, inverse_left, inverse_right):
    current = current.at[:, left_atom].add(-shift_term * inverse_left, mode="drop")
    return current.at[:, right_atom].add(shift_term * inverse_right, mode="drop")


def neighbours(rims):
    blocks = []
    for first_off in (-1, 0, 1):
        for second_off in (-1, 0, 1):
            for third_off in (-1, 0, 1):
                blocks.append(jnp.roll(rims, (-first_off, -second_off, -third_off), axis=(0, 1, 2)))
    return jnp.concatenate(blocks, axis=4)


def sweep(anchor_ext, inverse_ext, moved_ext, bond_pairs):
    left_atom = bond_pairs[0]
    right_atom = bond_pairs[1]
    inverse_left = inverse_ext[left_atom]
    inverse_right = inverse_ext[right_atom]
    shift_term, deviation = bond_terms(anchor_ext[:, left_atom], anchor_ext[:, right_atom],
                                       moved_ext[:, left_atom], moved_ext[:, right_atom],
                                       inverse_left, inverse_right)
    atoms = moved_ext.shape[1] - 27 * BOUND
    owned = moved_ext[:, :atoms]
    return apply_terms(owned, shift_term, left_atom, right_atom, inverse_left, inverse_right), deviation


def reference(ref_pos, step, inv_mass, boundary, bonds):
    edge_rows = (boundary + jnp.arange(BOUND, dtype=jnp.int32)[None, None, None, :]).astype(jnp.int32)

    def extend(values_in):
        picker = jnp.broadcast_to(edge_rows[:, :, :, None, :],
                                  values_in.shape[:4] + (BOUND,))
        rims = jnp.take_along_axis(values_in, picker, axis=4)
        whole = jnp.concatenate([values_in, neighbours(rims)], axis=4)
        return whole.reshape((-1,) + whole.shape[3:])

    anchor_ext = extend(ref_pos)
    inverse_ext = extend(inv_mass[:, :, :, None, :])[:, 0]
    bond_flat = bonds.reshape((-1,) + bonds.shape[3:])
    current = ref_pos + step
    reports = []
    for iteration in range(ITERS):
        moved_ext = extend(current)
        updated, deviation = jax.vmap(sweep)(anchor_ext, inverse_ext, moved_ext, bond_flat)
        current = updated.reshape(current.shape)
        reports.append(jnp.max(deviation))
    return current, jnp.stack(reports).astype(jnp.float32)
```

```python
import functools

import jax
import jax.numpy as jnp
from jax import lax
from jax.experimental import pallas as pl
from jax.experimental.pallas import tpu as pltpu
from jax.sharding import PartitionSpec as P

BOUND = 2048
CROSS_BONDS = 4096
ITERS = 3
CHAIN = 128
RELAX = 0.7
MESH = pl.DeviceIdType.MESH


def offsets(count):
    return (0, 1) if count == 2 else (-1, 0, 1)


def next_lane(x):
    return pltpu.roll(x, CHAIN - 1, x.ndim - 1)


def prev_lane(x):
    return pltpu.roll(x, 1, x.ndim - 1)


def dot3(a, b):
    return a[0] * b[0] + a[1] * b[1] + a[2] * b[2]


def bond_static(rest, weight):
    rest_sq = dot3(rest, rest)
    return rest_sq, 0.5 / jnp.maximum(rest_sq, 1.0), (0.5 * RELAX) / weight


def bond_force(rest, now, static):
    rest_sq, dev_scale, relax = static
    excess = dot3(now, now) - rest_sq
    force = relax * excess / jnp.maximum(dot3(rest, now), 1.0)
    return force, jnp.abs(excess) * dev_scale


def shifted(v, count, stride, off):
    rows = v.shape[0]
    if off == 0 or count == 1:
        return v
    row = lax.broadcasted_iota(jnp.int32, v.shape, 0)
    place = row // stride % count
    if off > 0:
        near = pltpu.roll(v, rows - stride, 0)
        if count * stride == rows:
            return near
        return jnp.where(place < count - 1, near, pltpu.roll(v, (count - 1) * stride, 0))
    near = pltpu.roll(v, stride, 0)
    if count * stride == rows:
        return near
    return jnp.where(place > 0, near, pltpu.roll(v, rows - (count - 1) * stride, 0))


def fetch(planes, codes, grid):
    gx, gy, gz = grid
    picked = [[None] * len(planes) for _ in codes]
    for dz in offsets(gz):
        moved_z = [shifted(v, gz, 1, dz) for v in planes]
        for dy in offsets(gy):
            moved_y = [shifted(v, gy, gz, dy) for v in moved_z]
            for dx in offsets(gx):
                if dx == 0 and dy == 0 and dz == 0:
                    continue
                moved = [shifted(v, gx, gy * gz, dx) for v in moved_y]
                number = float((dx + 1) * 9 + (dy + 1) * 3 + dz + 1)
                for which, code in enumerate(codes):
                    hit = code == number
                    for k, v in enumerate(moved):
                        old = picked[which][k]
                        picked[which][k] = v if old is None else jnp.where(hit, v, old)
    return picked


def chain_setup(anchor, inverse):
    lane = lax.broadcasted_iota(jnp.int32, inverse.shape, 1)
    rest = [a - next_lane(a) for a in anchor]
    static = bond_static(rest, inverse + next_lane(inverse))
    live = lane < CHAIN - 1
    rest_sq, dev_scale, relax = static
    zero = jnp.zeros_like(relax)
    return rest, (rest_sq, jnp.where(live, dev_scale, zero), jnp.where(live, relax, zero))


def chain_delta(moved, rest, static, inverse):
    now = [m - next_lane(m) for m in moved]
    force, dev = bond_force(rest, now, static)
    delta = []
    for c in range(3):
        term = force * rest[c]
        delta.append((prev_lane(term) - term) * inverse)
    return delta, dev


def full_max(x):
    return jnp.max(jnp.max(x, axis=0, keepdims=True), axis=1, keepdims=True)


def dev_row(devs):
    lane = lax.broadcasted_iota(jnp.int32, (1, CHAIN), 1)
    out = jnp.zeros((1, CHAIN), jnp.float32)
    for t, d in enumerate(devs):
        out = jnp.where(lane == t, full_max(d), out)
    return out


def kernel(grid, chains, start_ref, anchor_ref, step_ref, inv_ref, code_ref, out_ref, dev_ref,
           send, recv, res, back, send_sem, recv_sem, ret_sem, back_sem):
    gx, gy, gz = grid
    devices = gx * gy * gz
    share = devices // chains
    me = (lax.axis_index("gx") * gy + lax.axis_index("gy")) * gz + lax.axis_index("gz")
    line = me // gz
    is_owner = line % share == share - 1
    my_chain = line // share * gz + me % gz

    def coords(index):
        return (index // (gy * gz), index // gz % gy, index % gz)

    def owner_of(chain):
        return (chain // gz * share + share - 1) * gz + chain % gz

    barrier = pltpu.get_barrier_semaphore()

    def greet(k, carry):
        other = lax.rem(me + k, devices)
        pl.semaphore_signal(barrier, inc=1, device_id=coords(other), device_id_type=MESH)
        return carry

    lax.fori_loop(1, devices, greet, 0)

    start = jnp.full((chains, CHAIN), start_ref[0], jnp.int32)
    total_rows = inv_ref.shape[0]
    blocks = range(total_rows // chains)
    at = [start == g * BOUND for g in blocks]

    def edge(plane):
        out = plane(pl.ds(0, chains))
        for g in blocks[1:]:
            out = jnp.where(at[g], plane(pl.ds(g * chains, chains)), out)
        return out

    send_flat = send.reshape(send.shape[0] * chains, CHAIN)
    for c in range(3):
        a = edge(lambda rows: anchor_ref[c, rows, :])
        send_flat[c * chains:(c + 1) * chains, :] = a
        send_flat[(3 + c) * chains:(4 + c) * chains, :] = a + edge(lambda rows: step_ref[c, rows, :])
    send_flat[6 * chains:7 * chains, :] = edge(lambda rows: inv_ref[rows, :])
    send_flat[7 * chains:8 * chains, :] = code_ref[0]
    send_flat[8 * chains:9 * chains, :] = code_ref[1]

    group = 2 * chains
    devs = [jnp.zeros((8, CHAIN), jnp.float32)] * ITERS
    for base in range(0, total_rows, group):
        rows = pl.ds(base, group)
        anchor = [anchor_ref[c, rows, :] for c in range(3)]
        inverse = inv_ref[rows, :]
        moved = [anchor[c] + step_ref[c, rows, :] for c in range(3)]
        rest, static = chain_setup(anchor, inverse)
        inner = jnp.concatenate([start != base // chains * BOUND, start != (base // chains + 1) * BOUND], axis=0)
        for t in range(ITERS):
            delta, dev = chain_delta(moved, rest, static, inverse)
            dev = jnp.where(inner, dev, 0.0)
            devs[t] = jnp.maximum(devs[t], jnp.max(dev.reshape(group // 8, 8, CHAIN), axis=0))
            moved = [m + d for m, d in zip(moved, delta)]
        for c in range(3):
            out_ref[c, rows, :] = moved[c]
    send_flat[9 * chains:10 * chains, :] = jnp.broadcast_to(dev_row(devs), (chains, CHAIN))

    pl.semaphore_wait(barrier, devices - 1)

    def forward(chain):
        return pltpu.make_async_remote_copy(
            src_ref=send.at[:, chain], dst_ref=recv.at[:, me],
            send_sem=send_sem.at[chain], recv_sem=recv_sem.at[me],
            device_id=coords(owner_of(chain)), device_id_type=MESH)

    def backward(device):
        return pltpu.make_async_remote_copy(
            src_ref=res.at[:, device], dst_ref=back.at[:, my_chain],
            send_sem=ret_sem.at[device], recv_sem=back_sem.at[my_chain],
            device_id=coords(device), device_id_type=MESH)

    def send_chain(k, carry):
        chain = lax.rem(my_chain + k, chains)

        @pl.when(owner_of(chain) != me)
        def _():
            forward(chain).start()

        return carry

    lax.fori_loop(0, chains, send_chain, 0)

    @pl.when(is_owner)
    def _():
        recv[:, me] = send[:, my_chain]

        def arrive(k, carry):
            other = lax.rem(me + k, devices)
            pltpu.make_async_remote_copy(
                src_ref=send.at[:, 0], dst_ref=recv.at[:, other],
                send_sem=send_sem.at[0], recv_sem=recv_sem.at[other],
                device_id=coords(other), device_id_type=MESH).wait_recv()
            return carry

        lax.fori_loop(1, devices, arrive, 0)
        flat = recv.reshape(recv.shape[0] * devices, CHAIN)
        plane = [flat[k * devices:(k + 1) * devices, :] for k in range(10)]
        anchor, moved, inverse, codes, far_dev = plane[:3], plane[3:6], plane[6], plane[7:9], plane[9]
        rest, static = chain_setup(anchor, inverse)
        far = fetch(anchor + [inverse] + moved, codes, grid)
        cross = []
        for f in far:
            cross_rest = [a - b for a, b in zip(anchor, f[:3])]
            cross.append((cross_rest, bond_static(cross_rest, inverse + f[3])))
        far_moved = [f[4:] for f in far]
        tops = []
        for t in range(ITERS):
            if t:
                far_moved = fetch(moved, codes, grid)
            delta, top = chain_delta(moved, rest, static, inverse)
            for (cross_rest, cross_static), other in zip(cross, far_moved):
                now = [m - o for m, o in zip(moved, other)]
                force, dev = bond_force(cross_rest, now, cross_static)
                top = jnp.maximum(top, dev)
                pull = force * inverse
                delta = [d - pull * r for d, r in zip(delta, cross_rest)]
            moved = [m + d for m, d in zip(moved, delta)]
            tops.append(top)
        row = jnp.maximum(dev_row(tops), jnp.max(far_dev, axis=0, keepdims=True))
        res_flat = res.reshape(4 * devices, CHAIN)
        for c in range(3):
            res_flat[c * devices:(c + 1) * devices, :] = moved[c]
        res_flat[3 * devices:4 * devices, :] = jnp.broadcast_to(row, (devices, CHAIN))

        def give(k, carry):
            backward(lax.rem(me + k, devices)).start()
            return carry

        lax.fori_loop(1, devices, give, 0)
        back[:, my_chain] = res[:, me]

    def collect(k, carry):
        chain = lax.rem(my_chain + k, chains)

        @pl.when(owner_of(chain) != me)
        def _():
            pltpu.make_async_remote_copy(
                src_ref=res.at[:, 0], dst_ref=back.at[:, chain],
                send_sem=ret_sem.at[0], recv_sem=back_sem.at[chain],
                device_id=coords(owner_of(chain)), device_id_type=MESH).wait_recv()
            forward(chain).wait_send()

        return carry

    lax.fori_loop(0, chains, collect, 0)
    back_flat = back.reshape(4 * chains, CHAIN)
    edges = [back_flat[c * chains:(c + 1) * chains, :] for c in range(3)]
    top = jnp.max(back_flat[3 * chains:4 * chains, :], axis=0, keepdims=True)
    dev_ref[...] = jnp.broadcast_to(top, dev_ref.shape)
    for g in blocks:
        rows = pl.ds(g * chains, chains)
        for c in range(3):
            out_ref[c, rows, :] = jnp.where(at[g], edges[c], out_ref[c, rows, :])

    @pl.when(is_owner)
    def _():
        def finish(k, carry):
            backward(lax.rem(me + k, devices)).wait_send()
            return carry

        lax.fori_loop(1, devices, finish, 0)


def local(grid, ref_pos, step, inv_mass, boundary, bonds):
    atoms = ref_pos.shape[-1]
    rows = atoms // CHAIN
    chains = BOUND // CHAIN
    groups = CROSS_BONDS // BOUND
    devices = grid[0] * grid[1] * grid[2]
    ids = (bonds[0, 0, 0, 1, bonds.shape[-1] - CROSS_BONDS:] - atoms) // BOUND
    if grid[0] == 2:
        ids = jnp.where(ids < 9, ids + 18, ids)
    if grid[1] == 2:
        ids = jnp.where(ids // 3 % 3 == 0, ids + 6, ids)
    if grid[2] == 2:
        ids = jnp.where(ids % 3 == 0, ids + 2, ids)
    codes = ids.astype(jnp.float32).reshape(groups, chains, CHAIN)
    vmem = pl.BlockSpec(memory_space=pltpu.VMEM)
    f32 = jnp.float32
    out, dev = pl.pallas_call(
        functools.partial(kernel, grid, chains),
        out_shape=(jax.ShapeDtypeStruct((3, rows, CHAIN), f32),
                   jax.ShapeDtypeStruct((8, CHAIN), f32)),
        in_specs=[pl.BlockSpec(memory_space=pltpu.SMEM)] + [vmem] * 4,
        out_specs=(vmem, vmem),
        scratch_shapes=[
            pltpu.VMEM((10, chains, 1, CHAIN), f32),
            pltpu.VMEM((10, devices, 1, CHAIN), f32),
            pltpu.VMEM((4, devices, 1, CHAIN), f32),
            pltpu.VMEM((4, chains, 1, CHAIN), f32),
            pltpu.SemaphoreType.DMA((chains,)),
            pltpu.SemaphoreType.DMA((devices,)),
            pltpu.SemaphoreType.DMA((devices,)),
            pltpu.SemaphoreType.DMA((chains,)),
        ],
        compiler_params=pltpu.CompilerParams(collective_id=0, has_side_effects=True),
        name="bond_rounds",
    )(boundary[0, 0, 0], ref_pos[0, 0, 0].reshape(3, rows, CHAIN),
      step[0, 0, 0].reshape(3, rows, CHAIN), inv_mass[0, 0, 0].reshape(rows, CHAIN), codes)
    return out.reshape(1, 1, 1, 3, atoms), dev[0, :ITERS]


def solution(mesh):
    grid = (mesh.shape["gx"], mesh.shape["gy"], mesh.shape["gz"])
    return jax.shard_map(
        functools.partial(local, grid),
        mesh=mesh,
        in_specs=(
            P("gx", "gy", "gz", None, None),
            P("gx", "gy", "gz", None, None),
            P("gx", "gy", "gz", None),
            P("gx", "gy", "gz", None),
            P("gx", "gy", "gz", None, None),
        ),
        out_specs=(P("gx", "gy", "gz", None, None), P()),
        check_vma=False,
    )
```

```python
import functools

import jax
import jax.numpy as jnp
from jax import lax
from jax.experimental import pallas as pl
from jax.experimental.pallas import tpu as pltpu
from jax.sharding import PartitionSpec as P

BOUND = 2048
CROSS_BONDS = 4096
ITERS = 3
CHAIN = 128
RELAX = 0.7
LIMIT = 24 << 20
MESH = pl.DeviceIdType.MESH


def offsets(count):
    return (0, 1) if count == 2 else (-1, 0, 1)


def next_lane(x):
    return pltpu.roll(x, CHAIN - 1, x.ndim - 1)


def prev_lane(x):
    return pltpu.roll(x, 1, x.ndim - 1)


def dot3(a, b):
    return a[0] * b[0] + a[1] * b[1] + a[2] * b[2]


def bond_static(rest, weight):
    rest_sq = dot3(rest, rest)
    return rest_sq, 0.5 / jnp.maximum(rest_sq, 1.0), (0.5 * RELAX) / weight


def bond_force(rest, now, static):
    rest_sq, dev_scale, relax = static
    excess = dot3(now, now) - rest_sq
    force = relax * excess / jnp.maximum(dot3(rest, now), 1.0)
    return force, jnp.abs(excess) * dev_scale


def shifted(v, count, stride, off):
    rows = v.shape[0]
    if off == 0 or count == 1:
        return v
    row = lax.broadcasted_iota(jnp.int32, v.shape, 0)
    place = row // stride % count
    if off > 0:
        near = pltpu.roll(v, rows - stride, 0)
        if count * stride == rows:
            return near
        return jnp.where(place < count - 1, near, pltpu.roll(v, (count - 1) * stride, 0))
    near = pltpu.roll(v, stride, 0)
    if count * stride == rows:
        return near
    return jnp.where(place > 0, near, pltpu.roll(v, rows - (count - 1) * stride, 0))


def fetch(planes, codes, grid):
    gx, gy, gz = grid
    picked = [[None] * len(planes) for _ in codes]
    for dz in offsets(gz):
        moved_z = [shifted(v, gz, 1, dz) for v in planes]
        for dy in offsets(gy):
            moved_y = [shifted(v, gy, gz, dy) for v in moved_z]
            for dx in offsets(gx):
                if dx == 0 and dy == 0 and dz == 0:
                    continue
                moved = [shifted(v, gx, gy * gz, dx) for v in moved_y]
                number = float((dx + 1) * 9 + (dy + 1) * 3 + dz + 1)
                for which, code in enumerate(codes):
                    hit = code == number
                    for k, v in enumerate(moved):
                        old = picked[which][k]
                        picked[which][k] = v if old is None else jnp.where(hit, v, old)
    return picked


def chain_setup(anchor, inverse):
    lane = lax.broadcasted_iota(jnp.int32, inverse.shape, 1)
    rest = [a - next_lane(a) for a in anchor]
    static = bond_static(rest, inverse + next_lane(inverse))
    live = lane < CHAIN - 1
    rest_sq, dev_scale, relax = static
    zero = jnp.zeros_like(relax)
    return rest, (rest_sq, jnp.where(live, dev_scale, zero), jnp.where(live, relax, zero))


def chain_delta(moved, rest, static, inverse):
    now = [m - next_lane(m) for m in moved]
    force, dev = bond_force(rest, now, static)
    delta = []
    for c in range(3):
        term = force * rest[c]
        delta.append((prev_lane(term) - term) * inverse)
    return delta, dev


def full_max(x):
    return jnp.max(jnp.max(x, axis=0, keepdims=True), axis=1, keepdims=True)


def dev_row(devs):
    lane = lax.broadcasted_iota(jnp.int32, (1, CHAIN), 1)
    out = jnp.zeros((1, CHAIN), jnp.float32)
    for t, d in enumerate(devs):
        out = jnp.where(lane == t, full_max(d), out)
    return out


def boundary_codes(ids, atoms, grid):
    code = lax.shift_right_logical(ids - atoms, BOUND.bit_length() - 1)
    if grid[0] == 2:
        code = jnp.where(code < 9, code + 18, code)
    if grid[1] == 2:
        code = jnp.where(lax.rem(lax.div(code, 3), 3) == 0, code + 6, code)
    if grid[2] == 2:
        code = jnp.where(lax.rem(code, 3) == 0, code + 2, code)
    return code.astype(jnp.float32)


def kernel(grid, chains, start_ref, anchor_hbm, step_hbm, inv_hbm, bonds_hbm, bulk_ref, edge_out,
           anchor_ref, step_ref, inv_ref, tail_ref, tail_rows,
           send, recv, res, back, dev_send, dev_recv,
           load_sem, send_sem, recv_sem, dsend_sem, drecv_sem, ret_sem, back_sem):
    gx, gy, gz = grid
    devices = gx * gy * gz
    share = devices // chains
    lines = chains // gz
    mine = [lax.axis_index(n) for n in ("gx", "gy", "gz")]
    line = mine[0] * gy + mine[1]
    me = line * gz + mine[2]
    my_line = lax.div(line, share)
    is_owner = lax.rem(line, share) == share - 1
    my_chain = my_line * gz + mine[2]
    ys = [lax.rem(mine[1] + d, gy) for d in range(gy)]
    zs = [lax.rem(mine[2] + d, gz) for d in range(gz)]
    targets = []
    for i in range(lines):
        to = lax.rem(my_line + i, lines)
        to_line = to * share + share - 1
        x, y = lax.div(to_line, gy), lax.rem(to_line, gy)
        for z in zs:
            targets.append((to * gz + z, (x, y, z)))

    def each_other(act):
        def plane(x, skip):
            for dy, y in enumerate(ys):
                for dz, z in enumerate(zs):
                    if not (skip and dy == 0 and dz == 0):
                        act((x * gy + y) * gz + z, (x, y, z))

        plane(mine[0], True)
        if gx == 2:
            plane(1 - mine[0], False)
        else:
            def step(d, carry):
                plane(lax.rem(mine[0] + d, gx), False)
                return carry

            lax.fori_loop(1, gx, step, 0)

    def each_owner(act):
        for k, (chain, where) in enumerate(targets):
            if k == 0:
                @pl.when(jnp.logical_not(is_owner))
                def _(chain=chain, where=where):
                    act(chain, where)
            else:
                act(chain, where)

    def remote(src, dst, ssem, rsem, where):
        return pltpu.make_async_remote_copy(src_ref=src, dst_ref=dst, send_sem=ssem, recv_sem=rsem,
                                            device_id=where, device_id_type=MESH)

    barrier = pltpu.get_barrier_semaphore()
    each_other(lambda other, where: pl.semaphore_signal(
        barrier, inc=1, device_id=where, device_id_type=MESH))

    lo = bonds_hbm.shape[1] - tail_ref.shape[1]
    loads = [
        pltpu.make_async_copy(bonds_hbm.at[:, pl.ds(lo, tail_ref.shape[1])], tail_ref, load_sem.at[0]),
        pltpu.make_async_copy(anchor_hbm, anchor_ref, load_sem.at[1]),
        pltpu.make_async_copy(step_hbm, step_ref, load_sem.at[2]),
        pltpu.make_async_copy(inv_hbm, inv_ref, load_sem.at[3]),
    ]
    for copy in loads:
        copy.start()

    start = jnp.full((chains, CHAIN), start_ref[0], jnp.int32)
    total_rows = inv_ref.shape[0]
    blocks = range(total_rows // chains)
    at = [start == g * BOUND for g in blocks]

    def edge(plane):
        out = plane(pl.ds(0, chains))
        for g in blocks[1:]:
            out = jnp.where(at[g], plane(pl.ds(g * chains, chains)), out)
        return out

    fields = send.shape[1]
    send_flat = send.reshape(chains * fields, CHAIN)

    def put(k, plane):
        send_flat[pl.ds(k, chains, stride=fields), :] = plane

    loads[0].wait()
    width = tail_ref.shape[1]
    full = width // CHAIN
    tail_rows[...] = jnp.zeros_like(tail_rows)
    for t in range(full):
        tail_rows[t, :] = tail_ref[1, t * CHAIN:(t + 1) * CHAIN]
    if width % CHAIN:
        tail_rows[full, 0:width % CHAIN] = tail_ref[1, full * CHAIN:width]
    shift = width - CROSS_BONDS
    count = 2 * chains
    ids = tail_rows[0:count, :]
    if shift:
        lane = lax.broadcasted_iota(jnp.int32, ids.shape, 1)
        ids = jnp.where(lane < CHAIN - shift, pltpu.roll(ids, CHAIN - shift, 1),
                        pltpu.roll(tail_rows[1:count + 1, :], CHAIN - shift, 1))
    codes = boundary_codes(ids, total_rows * CHAIN, grid)
    put(7, codes[:chains])
    put(8, codes[chains:])
    for copy in loads[1:]:
        copy.wait()
    for c in range(3):
        a = edge(lambda rows: anchor_ref[c, rows, :])
        put(c, a)
        put(3 + c, a + edge(lambda rows: step_ref[c, rows, :]))
    put(6, edge(lambda rows: inv_ref[rows, :]))

    def forward(chain, where):
        return remote(send.at[chain], recv.at[me], send_sem.at[chain], recv_sem.at[me], where)

    def forward_dev(chain, where):
        return remote(dev_send, dev_recv.at[me], dsend_sem.at[chain], drecv_sem.at[me], where)

    def backward(other, where):
        return remote(res.at[other], back.at[my_chain], ret_sem.at[other], back_sem.at[my_chain], where)

    pl.semaphore_wait(barrier, devices - 1)
    each_owner(lambda chain, where: forward(chain, where).start())

    group = 2 * chains
    devs = [jnp.zeros((8, CHAIN), jnp.float32)] * ITERS
    for base in range(0, total_rows, group):
        rows = pl.ds(base, group)
        anchor = [anchor_ref[c, rows, :] for c in range(3)]
        inverse = inv_ref[rows, :]
        moved = [anchor[c] + step_ref[c, rows, :] for c in range(3)]
        rest, static = chain_setup(anchor, inverse)
        inner = jnp.concatenate([start != base // chains * BOUND,
                                 start != (base // chains + 1) * BOUND], axis=0)
        for t in range(ITERS):
            delta, dev = chain_delta(moved, rest, static, inverse)
            dev = jnp.where(inner, dev, 0.0)
            devs[t] = jnp.maximum(devs[t], jnp.max(dev.reshape(group // 8, 8, CHAIN), axis=0))
            moved = [m + d for m, d in zip(moved, delta)]
        for c in range(3):
            bulk_ref[c, rows, :] = moved[c]
    own_dev = dev_row(devs)
    dev_send[...] = own_dev
    each_owner(lambda chain, where: forward_dev(chain, where).start())

    @pl.when(is_owner)
    def _():
        recv[me] = send[my_chain]
        each_other(lambda other, where: remote(
            send.at[0], recv.at[other], send_sem.at[0], recv_sem.at[other], where).wait_recv())
        flat = recv.reshape(devices * fields, CHAIN)
        plane = [flat[pl.ds(k, devices, stride=fields), :] for k in range(fields)]
        anchor, moved, inverse, codes = plane[:3], plane[3:6], plane[6], plane[7:9]
        rest, static = chain_setup(anchor, inverse)
        far = fetch(anchor + [inverse] + moved, codes, grid)
        cross = []
        for f in far:
            cross_rest = [a - b for a, b in zip(anchor, f[:3])]
            cross.append((cross_rest, bond_static(cross_rest, inverse + f[3])))
        far_moved = [f[4:] for f in far]
        tops = []
        for t in range(ITERS):
            if t:
                far_moved = fetch(moved, codes, grid)
            delta, top = chain_delta(moved, rest, static, inverse)
            for (cross_rest, cross_static), other in zip(cross, far_moved):
                now = [m - o for m, o in zip(moved, other)]
                force, dev = bond_force(cross_rest, now, cross_static)
                top = jnp.maximum(top, dev)
                pull = force * inverse
                delta = [d - pull * r for d, r in zip(delta, cross_rest)]
            moved = [m + d for m, d in zip(moved, delta)]
            tops.append(top)
        res_flat = res.reshape(devices * 4, CHAIN)
        for c in range(3):
            res_flat[pl.ds(c, devices, stride=4), :] = moved[c]
        row = jnp.maximum(dev_row(tops), own_dev)
        dev_recv[me] = own_dev
        each_other(lambda other, where: remote(
            dev_send, dev_recv.at[other], dsend_sem.at[0], drecv_sem.at[other], where).wait_recv())
        far_dev = dev_recv.reshape(devices, CHAIN)[...]
        row = jnp.maximum(row, jnp.max(far_dev, axis=0, keepdims=True))
        res_flat[pl.ds(3, devices, stride=4), :] = jnp.broadcast_to(row, (devices, CHAIN))
        each_other(lambda other, where: backward(other, where).start())
        back[my_chain] = res[me]

    each_owner(lambda chain, where: forward(chain, where).wait_send())
    each_owner(lambda chain, where: forward_dev(chain, where).wait_send())
    each_owner(lambda chain, where: remote(
        res.at[0], back.at[chain], ret_sem.at[0], back_sem.at[chain], where).wait_recv())
    back_flat = back.reshape(chains * 4, CHAIN)
    for c in range(4):
        edge_out[c] = back_flat[pl.ds(c, chains, stride=4), :]

    @pl.when(is_owner)
    def _():
        each_other(lambda other, where: backward(other, where).wait_send())


def place(start_ref, bulk_ref, edge_ref, out_ref, dev_ref):
    chains = edge_ref.shape[1]
    start = jnp.full((chains, CHAIN), start_ref[0], jnp.int32)
    for g in range(bulk_ref.shape[1] // chains):
        rows = pl.ds(g * chains, chains)
        for c in range(3):
            out_ref[c, rows, :] = jnp.where(start == g * BOUND, edge_ref[c], bulk_ref[c, rows, :])
    top = jnp.max(edge_ref[3], axis=0, keepdims=True)
    lane = lax.broadcasted_iota(jnp.int32, top.shape, 1)
    for t in range(ITERS):
        dev_ref[t] = jnp.max(jnp.where(lane == t, top, 0.0))


def local(grid, ref_pos, step, inv_mass, boundary, bonds):
    atoms = ref_pos.shape[-1]
    rows = atoms // CHAIN
    chains = BOUND // CHAIN
    devices = grid[0] * grid[1] * grid[2]
    bond_count = bonds.shape[-1]
    tail = bond_count - (bond_count - CROSS_BONDS) // CHAIN * CHAIN
    vmem = pl.BlockSpec(memory_space=pltpu.VMEM)
    smem = pl.BlockSpec(memory_space=pltpu.SMEM)
    hbm = pl.BlockSpec(memory_space=pltpu.HBM)
    f32 = jnp.float32
    dma = pltpu.SemaphoreType.DMA
    start = boundary[0, 0, 0]
    whole = jax.ShapeDtypeStruct((3, rows, CHAIN), f32)
    bulk, edges = pl.pallas_call(
        functools.partial(kernel, grid, chains),
        out_shape=(whole, jax.ShapeDtypeStruct((4, chains, CHAIN), f32)),
        in_specs=[smem] + [hbm] * 4,
        out_specs=(vmem, vmem),
        scratch_shapes=[
            pltpu.VMEM((3, rows, CHAIN), f32),
            pltpu.VMEM((3, rows, CHAIN), f32),
            pltpu.VMEM((rows, CHAIN), f32),
            pltpu.VMEM((2, tail), jnp.int32),
            pltpu.VMEM((tail // CHAIN // 8 * 8 + 8, CHAIN), jnp.int32),
            pltpu.VMEM((chains, 9, 1, CHAIN), f32),
            pltpu.VMEM((devices, 9, 1, CHAIN), f32),
            pltpu.VMEM((devices, 4, 1, CHAIN), f32),
            pltpu.VMEM((chains, 4, 1, CHAIN), f32),
            pltpu.VMEM((1, CHAIN), f32),
            pltpu.VMEM((devices, 1, CHAIN), f32),
            dma((4,)), dma((chains,)), dma((devices,)), dma((chains,)), dma((devices,)),
            dma((devices,)), dma((chains,)),
        ],
        compiler_params=pltpu.CompilerParams(collective_id=0, has_side_effects=True,
                                             vmem_limit_bytes=LIMIT),
        name="bond_rounds",
    )(start, *(pltpu.with_memory_space_constraint(v, pltpu.HBM) for v in (
        ref_pos[0, 0, 0].reshape(3, rows, CHAIN), step[0, 0, 0].reshape(3, rows, CHAIN),
        inv_mass[0, 0, 0].reshape(rows, CHAIN), bonds[0, 0, 0])))
    out, dev = pl.pallas_call(
        place,
        out_shape=(whole, jax.ShapeDtypeStruct((ITERS,), f32)),
        in_specs=[smem, vmem, vmem],
        out_specs=(vmem, smem),
        compiler_params=pltpu.CompilerParams(vmem_limit_bytes=LIMIT),
        name="place_edges",
    )(start, bulk, edges)
    return out.reshape(1, 1, 1, 3, atoms), dev


def solution(mesh):
    grid = (mesh.shape["gx"], mesh.shape["gy"], mesh.shape["gz"])
    return jax.shard_map(
        functools.partial(local, grid),
        mesh=mesh,
        in_specs=(
            P("gx", "gy", "gz", None, None),
            P("gx", "gy", "gz", None, None),
            P("gx", "gy", "gz", None),
            P("gx", "gy", "gz", None),
            P("gx", "gy", "gz", None, None),
        ),
        out_specs=(P("gx", "gy", "gz", None, None), P()),
        check_vma=False,
    )
```

```python
import functools

import jax
import jax.numpy as jnp
from jax import lax
from jax.experimental import pallas as pl
from jax.experimental.pallas import tpu as pltpu
from jax.sharding import PartitionSpec as P

BOUND = 2048
CROSS_BONDS = 4096
ITERS = 3
CHAIN = 128
RELAX = 0.7
LIMIT = 24 << 20
MESH = pl.DeviceIdType.MESH


def offsets(count):
    return (0, 1) if count == 2 else (-1, 0, 1)


def next_lane(x):
    return pltpu.roll(x, CHAIN - 1, x.ndim - 1)


def prev_lane(x):
    return pltpu.roll(x, 1, x.ndim - 1)


def dot3(a, b):
    return a[0] * b[0] + a[1] * b[1] + a[2] * b[2]


def bond_static(rest, weight):
    rest_sq = dot3(rest, rest)
    return rest_sq, 0.5 / jnp.maximum(rest_sq, 1.0), (0.5 * RELAX) / weight


def bond_force(rest, now, static):
    rest_sq, dev_scale, relax = static
    excess = dot3(now, now) - rest_sq
    force = relax * excess / jnp.maximum(dot3(rest, now), 1.0)
    return force, jnp.abs(excess) * dev_scale


def shifted(v, count, stride, off):
    rows = v.shape[0]
    if off == 0 or count == 1:
        return v
    row = lax.broadcasted_iota(jnp.int32, v.shape, 0)
    place = row // stride % count
    if off > 0:
        near = pltpu.roll(v, rows - stride, 0)
        if count * stride == rows:
            return near
        return jnp.where(place < count - 1, near, pltpu.roll(v, (count - 1) * stride, 0))
    near = pltpu.roll(v, stride, 0)
    if count * stride == rows:
        return near
    return jnp.where(place > 0, near, pltpu.roll(v, rows - (count - 1) * stride, 0))


def fetch(planes, codes, grid):
    gx, gy, gz = grid
    picked = [[None] * len(planes) for _ in codes]
    for dz in offsets(gz):
        moved_z = [shifted(v, gz, 1, dz) for v in planes]
        for dy in offsets(gy):
            moved_y = [shifted(v, gy, gz, dy) for v in moved_z]
            for dx in offsets(gx):
                if dx == 0 and dy == 0 and dz == 0:
                    continue
                moved = [shifted(v, gx, gy * gz, dx) for v in moved_y]
                number = float((dx + 1) * 9 + (dy + 1) * 3 + dz + 1)
                for which, code in enumerate(codes):
                    hit = code == number
                    for k, v in enumerate(moved):
                        old = picked[which][k]
                        picked[which][k] = v if old is None else jnp.where(hit, v, old)
    return picked


def chain_setup(anchor, inverse):
    lane = lax.broadcasted_iota(jnp.int32, inverse.shape, 1)
    rest = [a - next_lane(a) for a in anchor]
    static = bond_static(rest, inverse + next_lane(inverse))
    live = lane < CHAIN - 1
    rest_sq, dev_scale, relax = static
    zero = jnp.zeros_like(relax)
    return rest, (rest_sq, jnp.where(live, dev_scale, zero), jnp.where(live, relax, zero))


def chain_delta(moved, rest, static, inverse):
    now = [m - next_lane(m) for m in moved]
    force, dev = bond_force(rest, now, static)
    delta = []
    for c in range(3):
        term = force * rest[c]
        delta.append((prev_lane(term) - term) * inverse)
    return delta, dev


def full_max(x):
    return jnp.max(jnp.max(x, axis=0, keepdims=True), axis=1, keepdims=True)


def dev_row(devs):
    lane = lax.broadcasted_iota(jnp.int32, (1, CHAIN), 1)
    out = jnp.zeros((1, CHAIN), jnp.float32)
    for t, d in enumerate(devs):
        out = jnp.where(lane == t, full_max(d), out)
    return out


def boundary_codes(ids, atoms, grid):
    code = lax.shift_right_logical(ids - atoms, BOUND.bit_length() - 1)
    if grid[0] == 2:
        code = jnp.where(code < 9, code + 18, code)
    if grid[1] == 2:
        code = jnp.where(lax.rem(lax.div(code, 3), 3) == 0, code + 6, code)
    if grid[2] == 2:
        code = jnp.where(lax.rem(code, 3) == 0, code + 2, code)
    return code.astype(jnp.float32)


def kernel(grid, chains, start_ref, anchor_hbm, step_hbm, inv_hbm, bonds_hbm, bulk_ref, edge_out,
           anchor_ref, step_ref, inv_ref, tail_ref, tail_rows,
           send, recv, res, back, dev_send, dev_recv,
           load_sem, send_sem, recv_sem, dsend_sem, drecv_sem, ret_sem, back_sem):
    gx, gy, gz = grid
    devices = gx * gy * gz
    stride = max(1, gx * gy // chains)
    lines = gx * gy // stride
    per = chains // lines
    first = (gz - per) // 2
    mine = [lax.axis_index(n) for n in ("gx", "gy", "gz")]
    line = mine[0] * gy + mine[1]
    me = line * gz + mine[2]
    my_line = lax.div(line, stride)
    is_owner = jnp.logical_and(lax.rem(line, stride) == stride - 1,
                               jnp.logical_and(mine[2] >= first, mine[2] < first + per))
    my_chain = my_line * per + mine[2] - first
    ys = [lax.rem(mine[1] + d, gy) for d in range(gy)]
    zs = [lax.rem(mine[2] + d, gz) for d in range(gz)]
    targets = []
    for i in reversed(range(lines)):
        to = lax.rem(my_line + i, lines)
        to_line = to * stride + stride - 1
        x, y = lax.div(to_line, gy), lax.rem(to_line, gy)
        for j in range(per):
            z = first + lax.rem(mine[2] + j, per)
            targets.append((i, to * per + z - first, (x, y, z)))

    def each_other(act):
        def plane(x, skip):
            for dy, y in enumerate(ys):
                for dz, z in enumerate(zs):
                    if not (skip and dy == 0 and dz == 0):
                        act((x * gy + y) * gz + z, (x, y, z))

        plane(mine[0], True)
        if gx == 2:
            plane(1 - mine[0], False)
        else:
            def step(d, carry):
                plane(lax.rem(mine[0] + d, gx), False)
                return carry

            lax.fori_loop(1, gx, step, 0)

    def each_owner(act):
        for i, chain, where in targets:
            if i == 0:
                @pl.when(jnp.logical_not(jnp.logical_and(is_owner, where[2] == mine[2])))
                def _(chain=chain, where=where):
                    act(chain, where)
            else:
                act(chain, where)

    def remote(src, dst, ssem, rsem, where):
        return pltpu.make_async_remote_copy(src_ref=src, dst_ref=dst, send_sem=ssem, recv_sem=rsem,
                                            device_id=where, device_id_type=MESH)

    barrier = pltpu.get_barrier_semaphore()

    @pl.when(is_owner)
    def _():
        each_other(lambda other, where: pl.semaphore_signal(
            barrier, inc=1, device_id=where, device_id_type=MESH))


    lo = bonds_hbm.shape[1] - tail_ref.shape[1]
    loads = [
        pltpu.make_async_copy(bonds_hbm.at[:, pl.ds(lo, tail_ref.shape[1])], tail_ref, load_sem.at[0]),
        pltpu.make_async_copy(anchor_hbm, anchor_ref, load_sem.at[1]),
        pltpu.make_async_copy(step_hbm, step_ref, load_sem.at[2]),
        pltpu.make_async_copy(inv_hbm, inv_ref, load_sem.at[3]),
    ]
    for copy in loads:
        copy.start()

    start = jnp.full((chains, CHAIN), start_ref[0], jnp.int32)
    total_rows = inv_ref.shape[0]
    blocks = range(total_rows // chains)
    at = [start == g * BOUND for g in blocks]

    def edge(plane):
        out = plane(pl.ds(0, chains))
        for g in blocks[1:]:
            out = jnp.where(at[g], plane(pl.ds(g * chains, chains)), out)
        return out

    fields = send.shape[1]
    send_flat = send.reshape(chains * fields, CHAIN)

    def put(k, plane):
        send_flat[pl.ds(k, chains, stride=fields), :] = plane

    loads[0].wait()
    width = tail_ref.shape[1]
    full = width // CHAIN
    tail_rows[...] = jnp.zeros_like(tail_rows)
    for t in range(full):
        tail_rows[t, :] = tail_ref[1, t * CHAIN:(t + 1) * CHAIN]
    if width % CHAIN:
        tail_rows[full, 0:width % CHAIN] = tail_ref[1, full * CHAIN:width]
    shift = width - CROSS_BONDS
    count = 2 * chains
    ids = tail_rows[0:count, :]
    if shift:
        lane = lax.broadcasted_iota(jnp.int32, ids.shape, 1)
        ids = jnp.where(lane < CHAIN - shift, pltpu.roll(ids, CHAIN - shift, 1),
                        pltpu.roll(tail_rows[1:count + 1, :], CHAIN - shift, 1))
    codes = boundary_codes(ids, total_rows * CHAIN, grid)
    put(7, codes[:chains])
    put(8, codes[chains:])
    for copy in loads[1:]:
        copy.wait()
    for c in range(3):
        a = edge(lambda rows: anchor_ref[c, rows, :])
        put(c, a)
        put(3 + c, a + edge(lambda rows: step_ref[c, rows, :]))
    put(6, edge(lambda rows: inv_ref[rows, :]))

    def forward(chain, where):
        return remote(send.at[chain], recv.at[me], send_sem.at[chain], recv_sem.at[me], where)

    def forward_dev(chain, where):
        return remote(dev_send, dev_recv.at[me], dsend_sem.at[chain], drecv_sem.at[me], where)

    def backward(other, where):
        return remote(res.at[other], back.at[my_chain], ret_sem.at[other], back_sem.at[my_chain], where)

    pl.semaphore_wait(barrier, chains - is_owner.astype(jnp.int32))
    each_owner(lambda chain, where: forward(chain, where).start())

    group = 2 * chains
    devs = [jnp.zeros((8, CHAIN), jnp.float32)] * ITERS
    for base in range(0, total_rows, group):
        rows = pl.ds(base, group)
        anchor = [anchor_ref[c, rows, :] for c in range(3)]
        inverse = inv_ref[rows, :]
        moved = [anchor[c] + step_ref[c, rows, :] for c in range(3)]
        rest, static = chain_setup(anchor, inverse)
        inner = jnp.concatenate([start != base // chains * BOUND,
                                 start != (base // chains + 1) * BOUND], axis=0)
        for t in range(ITERS):
            delta, dev = chain_delta(moved, rest, static, inverse)
            dev = jnp.where(inner, dev, 0.0)
            devs[t] = jnp.maximum(devs[t], jnp.max(dev.reshape(group // 8, 8, CHAIN), axis=0))
            moved = [m + d for m, d in zip(moved, delta)]
        for c in range(3):
            bulk_ref[c, rows, :] = moved[c]
    own_dev = dev_row(devs)
    dev_send[...] = own_dev
    each_owner(lambda chain, where: forward_dev(chain, where).start())

    @pl.when(is_owner)
    def _():
        recv[me] = send[my_chain]
        each_other(lambda other, where: remote(
            send.at[0], recv.at[other], send_sem.at[0], recv_sem.at[other], where).wait_recv())
        flat = recv.reshape(devices * fields, CHAIN)
        plane = [flat[pl.ds(k, devices, stride=fields), :] for k in range(fields)]
        anchor, moved, inverse, codes = plane[:3], plane[3:6], plane[6], plane[7:9]
        rest, static = chain_setup(anchor, inverse)
        far = fetch(anchor + [inverse] + moved, codes, grid)
        cross = []
        for f in far:
            cross_rest = [a - b for a, b in zip(anchor, f[:3])]
            cross.append((cross_rest, bond_static(cross_rest, inverse + f[3])))
        far_moved = [f[4:] for f in far]
        tops = []
        for t in range(ITERS):
            if t:
                far_moved = fetch(moved, codes, grid)
            delta, top = chain_delta(moved, rest, static, inverse)
            for (cross_rest, cross_static), other in zip(cross, far_moved):
                now = [m - o for m, o in zip(moved, other)]
                force, dev = bond_force(cross_rest, now, cross_static)
                top = jnp.maximum(top, dev)
                pull = force * inverse
                delta = [d - pull * r for d, r in zip(delta, cross_rest)]
            moved = [m + d for m, d in zip(moved, delta)]
            tops.append(top)
        res_flat = res.reshape(devices * 4, CHAIN)
        for c in range(3):
            res_flat[pl.ds(c, devices, stride=4), :] = moved[c]
        row = jnp.maximum(dev_row(tops), own_dev)
        dev_recv[me] = own_dev
        each_other(lambda other, where: remote(
            dev_send, dev_recv.at[other], dsend_sem.at[0], drecv_sem.at[other], where).wait_recv())
        far_dev = dev_recv.reshape(devices, CHAIN)[...]
        row = jnp.maximum(row, jnp.max(far_dev, axis=0, keepdims=True))
        res_flat[pl.ds(3, devices, stride=4), :] = jnp.broadcast_to(row, (devices, CHAIN))
        each_other(lambda other, where: backward(other, where).start())
        back[my_chain] = res[me]

    each_owner(lambda chain, where: forward(chain, where).wait_send())
    each_owner(lambda chain, where: forward_dev(chain, where).wait_send())
    each_owner(lambda chain, where: remote(
        res.at[0], back.at[chain], ret_sem.at[0], back_sem.at[chain], where).wait_recv())
    back_flat = back.reshape(chains * 4, CHAIN)
    for c in range(4):
        edge_out[c] = back_flat[pl.ds(c, chains, stride=4), :]

    @pl.when(is_owner)
    def _():
        each_other(lambda other, where: backward(other, where).wait_send())


def place(start_ref, bulk_ref, edge_ref, out_ref, dev_ref):
    chains = edge_ref.shape[1]
    start = jnp.full((chains, CHAIN), start_ref[0], jnp.int32)
    for g in range(bulk_ref.shape[1] // chains):
        rows = pl.ds(g * chains, chains)
        for c in range(3):
            out_ref[c, rows, :] = jnp.where(start == g * BOUND, edge_ref[c], bulk_ref[c, rows, :])
    top = jnp.max(edge_ref[3], axis=0, keepdims=True)
    lane = lax.broadcasted_iota(jnp.int32, top.shape, 1)
    for t in range(ITERS):
        dev_ref[t] = jnp.max(jnp.where(lane == t, top, 0.0))


def local(grid, ref_pos, step, inv_mass, boundary, bonds):
    atoms = ref_pos.shape[-1]
    rows = atoms // CHAIN
    chains = BOUND // CHAIN
    devices = grid[0] * grid[1] * grid[2]
    bond_count = bonds.shape[-1]
    tail = bond_count - (bond_count - CROSS_BONDS) // CHAIN * CHAIN
    vmem = pl.BlockSpec(memory_space=pltpu.VMEM)
    smem = pl.BlockSpec(memory_space=pltpu.SMEM)
    hbm = pl.BlockSpec(memory_space=pltpu.HBM)
    f32 = jnp.float32
    dma = pltpu.SemaphoreType.DMA
    start = boundary[0, 0, 0]
    whole = jax.ShapeDtypeStruct((3, rows, CHAIN), f32)
    bulk, edges = pl.pallas_call(
        functools.partial(kernel, grid, chains),
        out_shape=(whole, jax.ShapeDtypeStruct((4, chains, CHAIN), f32)),
        in_specs=[smem] + [hbm] * 4,
        out_specs=(vmem, vmem),
        scratch_shapes=[
            pltpu.VMEM((3, rows, CHAIN), f32),
            pltpu.VMEM((3, rows, CHAIN), f32),
            pltpu.VMEM((rows, CHAIN), f32),
            pltpu.VMEM((2, tail), jnp.int32),
            pltpu.VMEM((tail // CHAIN // 8 * 8 + 8, CHAIN), jnp.int32),
            pltpu.VMEM((chains, 9, 1, CHAIN), f32),
            pltpu.VMEM((devices, 9, 1, CHAIN), f32),
            pltpu.VMEM((devices, 4, 1, CHAIN), f32),
            pltpu.VMEM((chains, 4, 1, CHAIN), f32),
            pltpu.VMEM((1, CHAIN), f32),
            pltpu.VMEM((devices, 1, CHAIN), f32),
            dma((4,)), dma((chains,)), dma((devices,)), dma((chains,)), dma((devices,)),
            dma((devices,)), dma((chains,)),
        ],
        compiler_params=pltpu.CompilerParams(collective_id=0, has_side_effects=True,
                                             vmem_limit_bytes=LIMIT),
        name="bond_rounds",
    )(start, *(pltpu.with_memory_space_constraint(v, pltpu.HBM) for v in (
        ref_pos[0, 0, 0].reshape(3, rows, CHAIN), step[0, 0, 0].reshape(3, rows, CHAIN),
        inv_mass[0, 0, 0].reshape(rows, CHAIN), bonds[0, 0, 0])))
    out, dev = pl.pallas_call(
        place,
        out_shape=(whole, jax.ShapeDtypeStruct((ITERS,), f32)),
        in_specs=[smem, vmem, vmem],
        out_specs=(vmem, smem),
        compiler_params=pltpu.CompilerParams(vmem_limit_bytes=LIMIT),
        name="place_edges",
    )(start, bulk, edges)
    return out.reshape(1, 1, 1, 3, atoms), dev


def solution(mesh):
    grid = (mesh.shape["gx"], mesh.shape["gy"], mesh.shape["gz"])
    return jax.shard_map(
        functools.partial(local, grid),
        mesh=mesh,
        in_specs=(
            P("gx", "gy", "gz", None, None),
            P("gx", "gy", "gz", None, None),
            P("gx", "gy", "gz", None),
            P("gx", "gy", "gz", None),
            P("gx", "gy", "gz", None, None),
        ),
        out_specs=(P("gx", "gy", "gz", None, None), P()),
        check_vma=False,
    )
```
